768 devices in a mesh: corpus: 192 (over x_hi, y, z), tensor: 4 (over x_lo, core).
Axes of the slice: x: 4 (x_hi: 2, x_lo: 2; x = x_hi * 2 + x_lo), y: 8, z: 12, core: 2. Of those that a mesh axis runs over, the one named last changes fastest.
Arguments:
- q_states: bfloat16 [12288, 4096], P('corpus', 'tensor'), may hold values from -90 to 90
- k_states: bfloat16 [12288, 1024], P('corpus', 'tensor'), may hold values from -9 to 9
- v_states: bfloat16 [12288, 1024], P('corpus', 'tensor'), may hold values from -6 to 6
- residual: bfloat16 [12288, 4096], P('corpus'), may hold values from -170 to 170
- out_weight: bfloat16 [4096, 4096], P('tensor'), may hold values from -0.09375 to 0.09375
- final_gain: float32 [4096], replicated, may hold values from 0.25 to 1.75
- passages: bfloat16 [196608, 4096], P(('corpus', 'tensor')), may hold values from -5 to 5
- lengths: int32 [768], P('corpus'), may hold values from 1 to 16
Outputs:
- scores: float32 [768, 196608], P(None, ('corpus', 'tensor'))
- log_norm: float32 [768], replicated
The draws below stay inside these ranges and needn't reach their ends.
All inputs are finite; a program needn't handle non-finite values.
Results may differ from the reference program's by a relative error of at most 0.0003.
The reference program's roundings to bfloat16 on the way (of `weights`, `context` and `embed`) count: a program that leaves them out, or rounds other values in their place, can miss the bound.
Values may be sent and summed in bfloat16 or wider, within the bound.
No kernel may reach another device: no remote copies, remote signals or barrier semaphores. Data moves between devices by JAX's collectives and lax.ppermute only.
A program may use at most 64 MiB of HBM per device.

```python
import math
import jax
import jax.numpy as jnp
from jax import lax

D = 4096
HEADS = 32
KV_HEADS = 8
HEAD_DIM = 128
SEQ = 16
QUERIES = 768
TOKENS = 12288
PASSAGES = 196608
Q_WIDTH = 4096
KV_WIDTH = 1024


def key_values(key):
    return jnp.clip(jax.random.normal(jax.random.fold_in(key, 2), (TOKENS, KV_HEADS * HEAD_DIM), jnp.float32), -6.0, 6.0)


def draw_k_states(key, part):
    drawn = key_values(key)
    return drawn.astype(jnp.bfloat16)


def draw_q_states(key, part):
    entries = jnp.clip(jax.random.normal(jax.random.fold_in(key, 3), (TOKENS, HEADS * HEAD_DIM), jnp.float32), -6.0, 6.0)
    return entries.astype(jnp.bfloat16)


def draw_residual(key, part):
    entries = jnp.clip(jax.random.normal(jax.random.fold_in(key, 1), (TOKENS, D), jnp.float32), -6.0, 6.0)
    return entries.astype(jnp.bfloat16)


def draw_passages(key, part):
    entries = jnp.clip(jax.random.normal(jax.random.fold_in(key, 5), (PASSAGES, D), jnp.float32), -6.0, 6.0) * 0.0625
    return entries.astype(jnp.bfloat16)


def plant(result, stream_key, least, high):
    place = [jax.random.randint(jax.random.fold_in(stream_key, axis), (), 0, length) for axis, length in enumerate(result.shape)]
    widest = result.shape.index(max(result.shape))
    neighbour = place[:widest] + [(place[widest] + 1) % result.shape[widest]] + place[widest + 1:]
    return result.at[tuple(place)].set(least).at[tuple(neighbour)].set(high)


def level_of(own_key, dims, shards, least, high):
    level = 1.0
    for position, blocks in shards:
        steps = jax.random.uniform(jax.random.fold_in(jax.random.fold_in(own_key, 6), position), (blocks,), jnp.float32, least / len(shards), high / len(shards))
        level = level * jnp.repeat(jnp.exp(steps), dims[position] // blocks).reshape((-1,) + (1,) * (len(dims) - 1 - position))
    return level


def bell_draw(stream_key, dims, scale, limit, cuts=(), held_as=jnp.bfloat16):
    gain = level_of(stream_key, dims, cuts, -0.22, 0.18) if cuts else 1.0
    values = jax.random.normal(stream_key, dims, jnp.float32) * scale * gain
    return jnp.minimum(jnp.maximum(values, -limit), limit).astype(held_as)


def setup_inputs(seed: int = 0) -> dict:
    arg_keys = jax.random.split(jax.random.key(seed), 9)
    return {
        "q_states": draw_q_states(jax.random.fold_in(arg_keys[8], 71), 0),
        "k_states": draw_k_states(jax.random.fold_in(arg_keys[8], 71), 0),
        "v_states": bell_draw(arg_keys[2], (TOKENS, KV_WIDTH), 1.0, 6.0, ((0, 192), (1, 4))),
        "residual": draw_residual(jax.random.fold_in(arg_keys[8], 71), 0),
        "out_weight": bell_draw(arg_keys[4], (Q_WIDTH, D), Q_WIDTH ** -0.5, 0.09375, ((0, 4),)),
        "final_gain": jnp.clip(1.0 + 0.15 * jax.random.normal(arg_keys[5], (D,), jnp.float32), 0.25, 1.75),
        "passages": draw_passages(jax.random.fold_in(arg_keys[8], 71), 0),
        "lengths": plant(jax.random.randint(arg_keys[7], (QUERIES,), 1, SEQ + 1), jax.random.fold_in(arg_keys[7], 1), 1, SEQ).astype(jnp.int32),
    }


score_scale = 50.0

def attend_rows(queries, key_rows, value_rows, query_place, lengths):
    query_count = queries.shape[0]
    query_span = queries.shape[1]
    pair_heads = key_rows.shape[2] // HEAD_DIM
    grouped = queries.astype(jnp.float32).reshape(query_count, query_span, pair_heads, -1, HEAD_DIM)
    keyed = key_rows.astype(jnp.float32).reshape(query_count, SEQ, pair_heads, HEAD_DIM)
    valued = value_rows.astype(jnp.float32).reshape(query_count, SEQ, pair_heads, HEAD_DIM)
    logits = jnp.einsum('brkgd,bskd->bkgrs', grouped, keyed) / math.sqrt(HEAD_DIM)
    key_place = lax.broadcasted_iota(jnp.int32, (1, 1, SEQ), 2)
    allowed = (key_place <= query_place[:, :, None]) & (key_place < lengths[:, None, None])
    allowed = allowed[:, None, None, :, :]
    logits = jnp.where(allowed, logits, -1e+30)
    highest = lax.optimization_barrier(jnp.max(logits, axis=-1, keepdims=True))
    weights = jnp.where(allowed, jnp.exp(logits - highest), 0.0)
    attention = (weights / lax.optimization_barrier(jnp.sum(weights, axis=-1, keepdims=True))).astype(jnp.bfloat16)
    context = jnp.einsum('bkgrs,bskd->brkgd', attention.astype(jnp.float32), valued)
    return context.reshape(query_count * query_span, -1).astype(jnp.bfloat16)

def reference(q_states, k_states, v_states, residual, out_weight, final_gain, passages, lengths):
    query_count = lengths.shape[0]
    places = lax.broadcasted_iota(jnp.int32, (query_count, SEQ), 1)
    context = attend_rows(q_states.reshape(query_count, SEQ, -1), k_states.reshape(query_count, SEQ, -1), v_states.reshape(query_count, SEQ, -1), places, lengths)
    attended = jnp.dot(context, out_weight, preferred_element_type=jnp.float32)
    hidden = residual.astype(jnp.float32) + attended
    picker = (places == (lengths - 1)[:, None]).astype(jnp.float32)
    pooled = lax.optimization_barrier(jnp.sum(picker[:, :, None] * hidden.reshape(query_count, SEQ, -1), axis=1))
    scaled = pooled * final_gain.astype(jnp.float32)[None, :]
    magnitude = jnp.maximum(jnp.sqrt(lax.optimization_barrier(jnp.sum(scaled * scaled, axis=1, keepdims=True))), 1.0)
    embed = (scaled / magnitude).astype(jnp.bfloat16)
    scores = jnp.dot(embed, passages.T, preferred_element_type=jnp.float32) * score_scale
    highest = lax.optimization_barrier(jnp.max(scores, axis=1))
    log_norm = highest + jnp.log(lax.optimization_barrier(jnp.sum(jnp.exp(scores - highest[:, None]), axis=1)))
    return (scores, log_norm)
```

```python
import functools
import math

import jax
import jax.numpy as jnp
from jax import lax
from jax.sharding import Mesh
from jax.sharding import PartitionSpec as P

HEAD_DIM = 128
SEQ = 16
XH, Y, Z, XL, C = "corpus_0", "corpus_1", "corpus_2", "tensor_0", "tensor_1"
TENSOR = (XL, C)
CORPUS = (XH, Y, Z)
CORPUS_TENSOR = (XH, Y, Z, XL, C)

score_scale = 50.0


def size_of(axes):
    return math.prod(lax.axis_size(axis) for axis in axes)


def to_all(shard, axes):
    length = size_of(axes)
    return lax.all_to_all(
        jnp.broadcast_to(shard[None], (length, *shard.shape)), axes, 0, 0, tiled=True
    )


def swap(array, axis):
    return lax.ppermute(array, axis, [(0, 1), (1, 0)])


def attend_rows(queries, key_rows, value_rows, query_place, lengths):
    query_count = queries.shape[0]
    query_span = queries.shape[1]
    pair_heads = key_rows.shape[2] // HEAD_DIM
    grouped = queries.reshape(query_count, query_span, pair_heads, -1, HEAD_DIM)
    keyed = key_rows.reshape(query_count, SEQ, pair_heads, HEAD_DIM)
    valued = value_rows.reshape(query_count, SEQ, pair_heads, HEAD_DIM)
    logits = jnp.einsum(
        "brkgd,bskd->bkgrs", grouped, keyed, preferred_element_type=jnp.float32
    ) / math.sqrt(HEAD_DIM)
    key_place = lax.broadcasted_iota(jnp.int32, (1, 1, SEQ), 2)
    allowed = (key_place <= query_place[:, :, None]) & (key_place < lengths[:, None, None])
    allowed = allowed[:, None, None, :, :]
    logits = jnp.where(allowed, logits, -1e30)
    highest = jnp.max(logits, axis=-1, keepdims=True)
    weights = jnp.where(allowed, jnp.exp(logits - highest), 0.0)
    attention = (weights / jnp.sum(weights, axis=-1, keepdims=True)).astype(jnp.bfloat16)
    context = jnp.einsum("bkgrs,bskd->brkgd", attention, valued, preferred_element_type=jnp.float32)
    return context.reshape(query_count * query_span, -1).astype(jnp.bfloat16)


def normalize_rows(pooled, final_gain):
    scaled = pooled * final_gain[None, :]
    magnitude = jnp.maximum(jnp.sqrt(jnp.sum(scaled * scaled, axis=1, keepdims=True)), 1.0)
    return (scaled / magnitude).astype(jnp.bfloat16)


def merge(peaks, totals, axes):
    peak = jnp.max(peaks, axis=axes, keepdims=True)
    total = jnp.sum(totals * jnp.exp(peaks - peak), axis=axes)
    return jnp.squeeze(peak, axes), total


def on_device(q_states, k_states, v_states, residual, out_weight, final_gain, passages, lengths):
    xh, y, z, xl, c = (lax.axis_size(axis) for axis in CORPUS_TENSOR)
    tensor = xl * c
    query_count = lengths.shape[0]
    width = out_weight.shape[1]
    rows = y * z
    places = lax.broadcasted_iota(jnp.int32, (query_count, SEQ), 1)
    picker = (places == (lengths - 1)[:, None]).astype(jnp.float32)
    key_rows = k_states.reshape(query_count, SEQ, -1)
    value_rows = v_states.reshape(query_count, SEQ, -1)
    chosen_query = jnp.sum(
        picker[:, :, None] * q_states.reshape(query_count, SEQ, -1).astype(jnp.float32), axis=1
    )
    chosen_query = chosen_query.astype(jnp.bfloat16)
    context = attend_rows(
        chosen_query[:, None, :], key_rows, value_rows, (lengths - 1)[:, None], lengths
    )
    partial_value = jnp.dot(context, out_weight, preferred_element_type=jnp.float32)
    residual_last = jnp.sum(
        picker[:, :, None] * residual.reshape(query_count, SEQ, -1).astype(jnp.float32), axis=1
    )
    first = lax.axis_index(TENSOR) == 0
    partial_value = partial_value + jnp.where(first, residual_last, 0.0)

    terms = jnp.broadcast_to(partial_value[None], (xh, tensor, width)).reshape(xh * tensor, width)
    terms = lax.all_to_all(terms, (XH, XL, C), 0, 0, tiled=True)
    pooled = jnp.sum(terms.reshape(xh, tensor, width), axis=1)
    embed = normalize_rows(pooled, final_gain)

    held, embed = lax.optimization_barrier((passages, embed))
    across = swap(held, XL)
    partner = swap(held, C)
    across_partner = swap(across, C)

    one_z = to_all(embed[0:1], (Z,))
    two_y = to_all(embed[1:2], (Y,))
    one = to_all(one_z.reshape(z, width), (Y,)).reshape(rows, width)
    two = to_all(two_y.reshape(y, width), (Z,)).reshape(rows, width)
    gathered = jnp.concatenate([one, two], axis=0)

    def score(block):
        return (
            lax.dot_general(
                gathered, block, (((1,), (1,)), ((), ())), preferred_element_type=jnp.float32
            )
            * score_scale
        )

    blocks = [[score(held), score(partner)], [score(across), score(across_partner)]]
    local_peak = functools.reduce(
        jnp.maximum, [jnp.max(s, axis=1) for pair in blocks for s in pair]
    )
    local_total = sum(
        jnp.sum(jnp.exp(s - local_peak[:, None]), axis=1) for pair in blocks for s in pair
    )

    me_xl, me_c = lax.axis_index(XL), lax.axis_index(C)
    outgoing = []
    for a in range(2):
        for b in range(2):
            pair = [jnp.where(me_c == b, p[0], p[1]) for p in blocks]
            outgoing.append(jnp.where(me_xl == a, pair[0], pair[1]))
    returned = lax.all_to_all(jnp.stack(outgoing), TENSOR, 0, 0, tiled=True)

    pairs = to_all(jnp.stack([local_peak, local_total]), (Z, C)).reshape(z, c, 2, xh * rows)
    peak, total = merge(pairs[:, :, 0], pairs[:, :, 1], 0)
    pairs = to_all(jnp.stack([peak, total]), (XH, Y, XL)).reshape(xh * y, xl, 2, c, xh * rows)
    peak, total = merge(pairs[:, :, 0], pairs[:, :, 1], 0)
    log_norm = (peak + jnp.log(total)).reshape(tensor, xh * rows)

    def ordered(values):
        tail = values.shape[2:]
        one = values[:, :rows].reshape(tensor, y, z, *tail)
        two = values[:, rows:].reshape(tensor, z, y, *tail).swapaxes(1, 2)
        return jnp.moveaxis(jnp.stack([one, two]), 1, 3).reshape(xh * rows * tensor, *tail)

    return ordered(returned), ordered(log_norm)


def solution(mesh):
    split = Mesh(mesh.devices.reshape(2, 8, 12, 2, 2), CORPUS_TENSOR)
    in_specs = (
        P(CORPUS, TENSOR),
        P(CORPUS, TENSOR),
        P(CORPUS, TENSOR),
        P(CORPUS, None),
        P(TENSOR, None),
        P(),
        P(CORPUS_TENSOR, None),
        P(CORPUS),
    )
    out_specs = (P(None, CORPUS_TENSOR), P())
    return jax.shard_map(
        on_device, mesh=split, in_specs=in_specs, out_specs=out_specs, check_vma=False
    )
```

```python
import math

import jax
import jax.numpy as jnp
from jax import lax
from jax.experimental import pallas as pl
from jax.experimental.pallas import tpu as pltpu
from jax.sharding import Mesh
from jax.sharding import PartitionSpec as P


HEAD_DIM = 128
SEQ = 16
XH, YH, YL, ZH, ZL, XL, C = "xh", "yh", "yl", "zh", "zl", "xl", "c"
TENSOR = (XL, C)
CORPUS = (XH, YH, YL, ZH, ZL)
CORPUS_TENSOR = (*CORPUS, *TENSOR)

score_scale = 50.0


def size_of(axes):
    return math.prod(lax.axis_size(axis) for axis in axes)


def to_all(shard, axes):
    length = size_of(axes)
    return lax.all_to_all(
        jnp.broadcast_to(shard[None], (length, *shard.shape)), axes, 0, 0, tiled=True
    )


def swap(array, axis):
    return lax.ppermute(array, axis, [(0, 1), (1, 0)])


def attend_rows(queries, key_rows, value_rows, query_place, lengths):
    query_count = queries.shape[0]
    query_span = queries.shape[1]
    pair_heads = key_rows.shape[2] // HEAD_DIM
    grouped = queries.reshape(query_count, query_span, pair_heads, -1, HEAD_DIM)
    keyed = key_rows.reshape(query_count, SEQ, pair_heads, HEAD_DIM)
    valued = value_rows.reshape(query_count, SEQ, pair_heads, HEAD_DIM)
    logits = jnp.einsum(
        "brkgd,bskd->bkgrs", grouped, keyed, preferred_element_type=jnp.float32
    ) / math.sqrt(HEAD_DIM)
    key_place = lax.broadcasted_iota(jnp.int32, (1, 1, SEQ), 2)
    allowed = (key_place <= query_place[:, :, None]) & (key_place < lengths[:, None, None])
    allowed = allowed[:, None, None, :, :]
    logits = jnp.where(allowed, logits, -1e30)
    highest = jnp.max(logits, axis=-1, keepdims=True)
    weights = jnp.where(allowed, jnp.exp(logits - highest), 0.0)
    attention = (weights / jnp.sum(weights, axis=-1, keepdims=True)).astype(jnp.bfloat16)
    context = jnp.einsum("bkgrs,bskd->brkgd", attention, valued, preferred_element_type=jnp.float32)
    return context.reshape(query_count * query_span, -1).astype(jnp.bfloat16)


def normalize_rows(pooled, final_gain):
    scaled = pooled * final_gain[None, :]
    magnitude = jnp.maximum(jnp.sqrt(jnp.sum(scaled * scaled, axis=1, keepdims=True)), 1.0)
    return (scaled / magnitude).astype(jnp.bfloat16)


def merge(peaks, totals, axes):
    peak = jnp.max(peaks, axis=axes, keepdims=True)
    total = jnp.sum(totals * jnp.exp(peaks - peak), axis=axes)
    return jnp.squeeze(peak, axes), total


def score_kernel(rows_ref, *refs):
    blocks, outs, (stats_ref, held, arrived) = refs[:4], refs[4:8], refs[8:]
    copies = [
        pltpu.make_async_copy(block, held.at[i], arrived.at[i]) for i, block in enumerate(blocks)
    ]
    for copy in copies:
        copy.start()
    count = rows_ref.shape[0]
    peak = None
    for i, out in enumerate(outs):
        copies[i].wait()
        scores = (
            lax.dot_general(
                rows_ref[...], held[i], (((1,), (1,)), ((), ())), preferred_element_type=jnp.float32
            )
            * score_scale
        )
        out[...] = scores
        top = jnp.max(scores, axis=1, keepdims=True)
        peak = top if peak is None else jnp.maximum(peak, top)
    total = sum(jnp.sum(jnp.exp(out[...] - peak), axis=1, keepdims=True) for out in outs)
    lane = lax.broadcasted_iota(jnp.int32, (count, 128), 1)
    both = jnp.where(lane == 0, peak, total)
    stats_ref[...] = jnp.transpose(both)[: stats_ref.shape[0]]


def score_blocks(rows, blocks):
    count, width = rows.shape
    passages = blocks[0].shape[0]
    space = pl.BlockSpec(memory_space=pltpu.VMEM)
    return pl.pallas_call(
        score_kernel,
        name="score_blocks",
        out_shape=[jax.ShapeDtypeStruct((count, passages), jnp.float32)] * 4
        + [jax.ShapeDtypeStruct((2, count), jnp.float32)],
        in_specs=[space] + [pl.BlockSpec(memory_space=pl.ANY)] * 4,
        out_specs=[space] * 5,
        scratch_shapes=[
            pltpu.VMEM((4, passages, width), jnp.bfloat16),
            pltpu.SemaphoreType.DMA((4,)),
        ],
        cost_estimate=pl.CostEstimate(
            flops=8 * count * passages * width,
            bytes_accessed=8 * passages * width,
            transcendentals=4 * count * passages,
        ),
    )(rows, *blocks)


def step(q_states, k_states, v_states, residual, out_weight, final_gain, passages, lengths):
    xh, yh, yl, zh, zl, xl, c = (lax.axis_size(axis) for axis in CORPUS_TENSOR)
    tensor = xl * c
    query_count = lengths.shape[0]
    width = out_weight.shape[1]
    rows = yh * yl * zh * zl * xh
    places = lax.broadcasted_iota(jnp.int32, (query_count, SEQ), 1)
    picker = (places == (lengths - 1)[:, None]).astype(jnp.float32)
    key_rows = k_states.reshape(query_count, SEQ, -1)
    value_rows = v_states.reshape(query_count, SEQ, -1)
    chosen_query = jnp.sum(
        picker[:, :, None] * q_states.reshape(query_count, SEQ, -1).astype(jnp.float32), axis=1
    )
    chosen_query = chosen_query.astype(jnp.bfloat16)
    context = attend_rows(
        chosen_query[:, None, :], key_rows, value_rows, (lengths - 1)[:, None], lengths
    )
    partial_value = jnp.dot(context, out_weight, preferred_element_type=jnp.float32)
    residual_last = jnp.sum(
        picker[:, :, None] * residual.reshape(query_count, SEQ, -1).astype(jnp.float32), axis=1
    )
    first = lax.axis_index(TENSOR) == 0
    partial_value = partial_value + jnp.where(first, residual_last, 0.0)

    terms = jnp.broadcast_to(partial_value[None], (xh, tensor, width)).reshape(xh * tensor, width)
    terms = lax.all_to_all(terms, (XH, XL, C), 0, 0, tiled=True)
    pooled = jnp.sum(terms.reshape(xh, tensor, width), axis=1)
    embed = normalize_rows(pooled, final_gain)

    held, embed = lax.optimization_barrier((passages, embed))
    across = swap(held, XL)
    partner = swap(held, C)
    both = swap(across, C)

    gathered = to_all(embed, (YH, ZH)).reshape(-1, width)
    gathered = to_all(gathered, (YL, ZL)).reshape(-1, width)

    *blocks, stats = score_blocks(gathered, (held, partner, across, both))

    own, for_partner, for_across, for_both = blocks
    from_partner = swap(for_partner, C)
    from_across = swap(for_across, XL)
    from_both = lax.ppermute(for_both, TENSOR, [(i, tensor - 1 - i) for i in range(tensor)])

    pairs = to_all(stats, (ZH, ZL, C))
    pairs = pairs.reshape(zh * zl, c, 2, rows)
    peak, total = merge(pairs[:, :, 0], pairs[:, :, 1], 0)
    pairs = to_all(jnp.stack([peak, total]), (XH, YH, YL, XL))
    pairs = pairs.reshape(xh * yh * yl, xl, 2, c, rows)
    peak, total = merge(pairs[:, :, 0], pairs[:, :, 1], 0)
    log_norm = (peak + jnp.log(total)).reshape(tensor, rows)

    me_xl, me_c = lax.axis_index(XL), lax.axis_index(C)
    here = [jnp.where(me_c == i, own, from_partner) for i in range(2)]
    there = [jnp.where(me_c == i, from_across, from_both) for i in range(2)]
    returned = jnp.stack(
        [jnp.where(me_xl == i // 2, here[i % 2], there[i % 2]) for i in range(tensor)]
    )

    def ordered(values):
        tail = values.shape[2:]
        values = values.reshape(tensor, yl, zl, yh, zh, xh, *tail)
        last = tuple(range(6, 6 + len(tail)))
        return values.transpose((5, 3, 1, 4, 2, 0, *last)).reshape(rows * tensor, *tail)

    return ordered(returned), ordered(log_norm)


def solution(mesh):
    split = Mesh(mesh.devices.reshape(2, 4, 2, 6, 2, 2, 2), CORPUS_TENSOR)
    in_specs = (
        P(CORPUS, TENSOR),
        P(CORPUS, TENSOR),
        P(CORPUS, TENSOR),
        P(CORPUS, None),
        P(TENSOR, None),
        P(),
        P(CORPUS_TENSOR, None),
        P(CORPUS),
    )
    out_specs = (P(None, CORPUS_TENSOR), P())
    return jax.shard_map(step, mesh=split, in_specs=in_specs, out_specs=out_specs, check_vma=False)
```

```python
import functools
import math

import jax
import jax.numpy as jnp
from jax import lax
from jax.experimental import pallas as pl
from jax.experimental.pallas import tpu as pltpu
from jax.sharding import Mesh
from jax.sharding import PartitionSpec as P


HEAD_DIM = 128
SEQ = 16
XH, YH, YL, ZH, ZL, XL, C = "xh", "yh", "yl", "zh", "zl", "xl", "c"
TENSOR = (XL, C)
CORPUS = (XH, YH, YL, ZH, ZL)
CORPUS_TENSOR = (*CORPUS, *TENSOR)

score_scale = 50.0


def size_of(axes):
    return math.prod(lax.axis_size(axis) for axis in axes)


def to_all(shard, axes):
    length = size_of(axes)
    return lax.all_to_all(
        jnp.broadcast_to(shard[None], (length, *shard.shape)), axes, 0, 0, tiled=True
    )


def swap(array, axis):
    return lax.ppermute(array, axis, [(0, 1), (1, 0)])


def project_kernel(lengths_ref, *refs):
    sources, (out_ref, q_ref, k_ref, v_ref, residual_ref, weight_ref, arrived) = refs[:5], refs[5:]
    chunks = weight_ref.shape[0]
    depth = weight_ref.shape[1]
    copies = [
        pltpu.make_async_copy(source, held, arrived.at[i])
        for i, (source, held) in enumerate(
            zip(sources[:4], (q_ref, k_ref, v_ref, residual_ref), strict=True)
        )
    ] + [
        pltpu.make_async_copy(
            sources[4].at[pl.ds(i * depth, depth)], weight_ref.at[i], arrived.at[4 + i]
        )
        for i in range(chunks)
    ]
    for copy in copies:
        copy.start()
    count = lengths_ref.shape[0]
    tokens = count * SEQ
    pair_heads = k_ref.shape[1] // HEAD_DIM
    shared = q_ref.shape[1] // HEAD_DIM // pair_heads
    rows = shared * count

    def last_of(query):
        place = jnp.zeros_like(query)
        for b in range(count):
            place = jnp.where(query == b, b * SEQ + lengths_ref[b] - 1, place)
        return place

    def one_hot(hit):
        return jnp.where(hit, 1.0, 0.0).astype(jnp.bfloat16)

    row = lax.broadcasted_iota(jnp.int32, (rows, tokens), 0)
    token = lax.broadcasted_iota(jnp.int32, (rows, tokens), 1)
    query = row % count
    last = last_of(query)
    allowed = (token >= query * SEQ) & (token <= last)
    picks = [one_hot((token == last) & (row // count == h)) for h in range(shared)]
    for copy in copies[:3]:
        copy.wait()
    total = out_ref.shape[0]
    slot = lax.broadcasted_iota(jnp.int32, (total, rows), 0)
    source_row = lax.broadcasted_iota(jnp.int32, (total, rows), 1)
    spread = [one_hot(source_row == h * count + slot % count) for h in range(shared)]
    parts = []
    for g in range(pair_heads):
        columns = pl.ds(g * HEAD_DIM, HEAD_DIM)
        queries = sum(
            jnp.dot(
                picks[h],
                q_ref[:, pl.ds((g * shared + h) * HEAD_DIM, HEAD_DIM)],
                preferred_element_type=jnp.float32,
            )
            for h in range(shared)
        ).astype(jnp.bfloat16)
        logits = lax.dot_general(
            queries, k_ref[:, columns], (((1,), (1,)), ((), ())), preferred_element_type=jnp.float32
        ) / math.sqrt(HEAD_DIM)
        logits = jnp.where(allowed, logits, -1e30)
        weights = jnp.where(
            allowed, jnp.exp(logits - jnp.max(logits, axis=1, keepdims=True)), 0.0
        )
        attention = (weights / jnp.sum(weights, axis=1, keepdims=True)).astype(jnp.bfloat16)
        context = jnp.dot(
            attention, v_ref[:, columns], preferred_element_type=jnp.float32
        ).astype(jnp.bfloat16)
        parts += [
            jnp.dot(spread[h], context, preferred_element_type=jnp.float32).astype(jnp.bfloat16)
            for h in range(shared)
        ]
    place = lax.broadcasted_iota(jnp.int32, (total, tokens), 1)
    owner = lax.broadcasted_iota(jnp.int32, (total, tokens), 0) % count
    first = lax.axis_index(XL) + lax.axis_index(C) == 0
    copies[3].wait()
    terms = jnp.dot(
        one_hot((place == last_of(owner)) & first),
        residual_ref[...],
        preferred_element_type=jnp.float32,
    )
    per = depth // HEAD_DIM
    for i in range(chunks):
        part = jnp.concatenate(parts[i * per : (i + 1) * per], axis=1)
        copies[4 + i].wait()
        terms = terms + jnp.dot(part, weight_ref[i], preferred_element_type=jnp.float32)
    out_ref[...] = terms


def project(q_states, k_states, v_states, residual, out_weight, lengths, total):
    depth, width = out_weight.shape
    chunks = 4
    whole = [q_states, k_states, v_states, residual]
    arrays = [pltpu.with_memory_space_constraint(x, pltpu.HBM) for x in (*whole, out_weight)]
    return pl.pallas_call(
        project_kernel,
        name="project",
        out_shape=jax.ShapeDtypeStruct((total, width), jnp.float32),
        in_specs=[pl.BlockSpec(memory_space=pltpu.SMEM)]
        + [pl.BlockSpec(memory_space=pltpu.HBM)] * 5,
        out_specs=pl.BlockSpec(memory_space=pltpu.VMEM),
        scratch_shapes=[pltpu.VMEM(x.shape, x.dtype) for x in whole]
        + [
            pltpu.VMEM((chunks, depth // chunks, width), out_weight.dtype),
            pltpu.SemaphoreType.DMA((4 + chunks,)),
        ],
        compiler_params=pltpu.CompilerParams(vmem_limit_bytes=24 * 1024 * 1024),
    )(lengths, *arrays)


def embed_kernel(terms_ref, gain_ref, out_ref):
    groups = out_ref.shape[1]
    per = terms_ref.shape[0] // groups
    rows = []
    for g in range(groups):
        pooled = terms_ref[g * per]
        for t in range(1, per):
            pooled = pooled + terms_ref[g * per + t]
        scaled = pooled * gain_ref[...]
        magnitude = jnp.maximum(jnp.sqrt(jnp.sum(scaled * scaled, axis=1, keepdims=True)), 1.0)
        rows.append(scaled / magnitude)
    embed = jnp.concatenate(rows, axis=0).astype(jnp.bfloat16)
    for slot in range(out_ref.shape[0]):
        out_ref[slot] = embed


def embed_rows(terms, final_gain, groups, copies):
    width = terms.shape[-1]
    space = pl.BlockSpec(memory_space=pltpu.VMEM)
    return pl.pallas_call(
        embed_kernel,
        name="embed_rows",
        out_shape=jax.ShapeDtypeStruct((copies, groups, width), jnp.bfloat16),
        in_specs=[space] * 2,
        out_specs=space,
        compiler_params=pltpu.CompilerParams(vmem_limit_bytes=8 * 1024 * 1024),
    )(terms, final_gain.reshape(1, width))


def merge(peaks, totals, axes):
    peak = jnp.max(peaks, axis=axes, keepdims=True)
    total = jnp.sum(totals * jnp.exp(peaks - peak), axis=axes)
    return jnp.squeeze(peak, axes), total


def score_kernel(rows_ref, *refs):
    blocks, (kept_ref, crossing_ref, stats_ref, held, arrived) = refs[:4], refs[4:]
    outs = [kept_ref.at[0], kept_ref.at[1], crossing_ref.at[0], crossing_ref.at[1]]
    copies = [
        pltpu.make_async_copy(block, held.at[i], arrived.at[i]) for i, block in enumerate(blocks)
    ]
    for copy in copies:
        copy.start()
    count = rows_ref.shape[0]
    peak = None
    for i, out in enumerate(outs):
        copies[i].wait()
        scores = (
            lax.dot_general(
                rows_ref[...], held[i], (((1,), (1,)), ((), ())), preferred_element_type=jnp.float32
            )
            * score_scale
        )
        out[...] = scores
        top = jnp.max(scores, axis=1, keepdims=True)
        peak = top if peak is None else jnp.maximum(peak, top)
    total = sum(jnp.sum(jnp.exp(out[...] - peak), axis=1, keepdims=True) for out in outs)
    lane = lax.broadcasted_iota(jnp.int32, (count, 128), 1)
    stats = jnp.transpose(jnp.where(lane == 0, peak, total))[:2]
    stats_ref[...] = jnp.broadcast_to(stats[None], stats_ref.shape)


def score_blocks(rows, blocks, copies):
    count, width = rows.shape
    passages = blocks[0].shape[0]
    space = pl.BlockSpec(memory_space=pltpu.VMEM)
    blocks = [pltpu.with_memory_space_constraint(block, pltpu.HBM) for block in blocks]
    return pl.pallas_call(
        score_kernel,
        name="score_blocks",
        out_shape=[jax.ShapeDtypeStruct((2, count, passages), jnp.float32)] * 2
        + [jax.ShapeDtypeStruct((copies, 2, count), jnp.float32)],
        in_specs=[space] + [pl.BlockSpec(memory_space=pltpu.HBM)] * 4,
        out_specs=[space] * 3,
        scratch_shapes=[
            pltpu.VMEM((4, passages, width), jnp.bfloat16),
            pltpu.SemaphoreType.DMA((4,)),
        ],
        cost_estimate=pl.CostEstimate(
            flops=8 * count * passages * width,
            bytes_accessed=8 * passages * width,
            transcendentals=4 * count * passages,
        ),
        compiler_params=pltpu.CompilerParams(vmem_limit_bytes=24 * 1024 * 1024),
    )(rows, *blocks)


def arrange_kernel(sizes, kept_ref, crossed_ref, given_ref, out_ref, by_owner, placed):
    xh, yh, yl, zh, zl, tensor = sizes
    me = lax.axis_index(XL) * 2 + lax.axis_index(C)
    for flip, ref in enumerate(
        (kept_ref.at[0], given_ref.at[0], crossed_ref.at[0], given_ref.at[1])
    ):
        for half in range(placed.shape[0]):
            by_owner[me ^ flip, half] = ref[:, pl.ds(half * 128, 128)]
    for t in range(tensor):
        for near in range(yl * zl):
            y0, z0 = near // zl, near % zl
            for y1 in range(yh):
                for x in range(xh):
                    start = (near * yh + y1) * zh * xh + x
                    to = ((x * yh + y1) * yl + y0) * zh * zl + z0
                    for half in range(placed.shape[0]):
                        placed[half, pl.ds(to * tensor + t, zh, stride=zl * tensor)] = by_owner[
                            t, half, pl.ds(start, zh, stride=xh)
                        ]
    for half in range(placed.shape[0]):
        out_ref[:, pl.ds(half * 128, 128)] = placed[half]


def arrange(kept, crossed, given, sizes):
    _, rows, passages = kept.shape
    tensor = sizes[-1]
    space = pl.BlockSpec(memory_space=pltpu.VMEM)
    return pl.pallas_call(
        functools.partial(arrange_kernel, sizes),
        name="arrange",
        out_shape=jax.ShapeDtypeStruct((rows * tensor, passages), jnp.float32),
        in_specs=[space] * 3,
        out_specs=space,
        scratch_shapes=[
            pltpu.VMEM((tensor, passages // 128, rows, 128), jnp.float32),
            pltpu.VMEM((passages // 128, rows * tensor, 128), jnp.float32),
        ],
        compiler_params=pltpu.CompilerParams(vmem_limit_bytes=8 * 1024 * 1024),
    )(kept, crossed, given)


def step(q_states, k_states, v_states, residual, out_weight, final_gain, passages, lengths):
    xh, yh, yl, zh, zl, xl, c = (lax.axis_size(axis) for axis in CORPUS_TENSOR)
    tensor = xl * c
    width = out_weight.shape[1]
    rows = yh * yl * zh * zl * xh
    terms = project(q_states, k_states, v_states, residual, out_weight, lengths, xh * tensor)

    terms = lax.all_to_all(
        terms.reshape(xh * tensor, 1, width), (XH, XL, C), 0, 0, tiled=True
    )

    across = swap(passages, XL)
    partner = swap(passages, C)
    both = swap(across, C)

    embed = embed_rows(terms, final_gain, xh, yh * zh)
    gathered = lax.all_to_all(embed, (YH, ZH), 0, 0, tiled=True).reshape(-1, width)
    gathered = to_all(gathered, (YL, ZL)).reshape(-1, width)

    kept, crossing, stats = score_blocks(
        gathered, (passages, partner, across, both), zh * zl * c
    )

    crossed = swap(crossing, XL)
    given = swap(jnp.stack([kept[1], crossed[1]]), C)
    scores = arrange(kept, crossed, given, (xh, yh, yl, zh, zl, tensor))

    pairs = lax.all_to_all(stats, (ZH, ZL, C), 0, 0, tiled=True)
    pairs = pairs.reshape(zh * zl, c, 2, rows)
    peak, total = merge(pairs[:, :, 0], pairs[:, :, 1], 0)
    pairs = to_all(jnp.stack([peak, total]), (XH, YH, YL, XL))
    pairs = pairs.reshape(xh * yh * yl, xl, 2, c, rows)
    peak, total = merge(pairs[:, :, 0], pairs[:, :, 1], 0)
    log_norm = (peak + jnp.log(total)).reshape(tensor, rows)

    log_norm = log_norm.reshape(tensor, yl, zl, yh, zh, xh).transpose(5, 3, 1, 4, 2, 0)
    return scores, log_norm.reshape(rows * tensor)


def solution(mesh):
    split = Mesh(mesh.devices.reshape(2, 4, 2, 6, 2, 2, 2), CORPUS_TENSOR)
    in_specs = (
        P(CORPUS, TENSOR),
        P(CORPUS, TENSOR),
        P(CORPUS, TENSOR),
        P(CORPUS, None),
        P(TENSOR, None),
        P(),
        P(CORPUS_TENSOR, None),
        P(CORPUS),
    )
    out_specs = (P(None, CORPUS_TENSOR), P())
    return jax.shard_map(step, mesh=split, in_specs=in_specs, out_specs=out_specs, check_vma=False)
```

```python
import functools
import math

import jax
import jax.numpy as jnp
from jax import lax
from jax.experimental import pallas as pl
from jax.experimental.pallas import tpu as pltpu
from jax.sharding import Mesh
from jax.sharding import PartitionSpec as P


HEAD_DIM = 128
SEQ = 16
XH, YH, YL, ZH, ZL, XL, C = "xh", "yh", "yl", "zh", "zl", "xl", "c"
TENSOR = (XL, C)
CORPUS = (XH, YH, YL, ZH, ZL)
CORPUS_TENSOR = (*CORPUS, *TENSOR)

score_scale = 50.0


def size_of(axes):
    return math.prod(lax.axis_size(axis) for axis in axes)


def to_all(shard, axes):
    length = size_of(axes)
    return lax.all_to_all(
        jnp.broadcast_to(shard[None], (length, *shard.shape)), axes, 0, 0, tiled=True
    )


def shifted(array, axes, along_y, along_z):
    y, z = size_of(axes[:2]), size_of(axes[2:])
    moves = [
        (i * z + j, (i + along_y) % y * z + (j + along_z) % z) for i in range(y) for j in range(z)
    ]
    return lax.ppermute(array, axes, moves)


def swap(array, axis):
    return lax.ppermute(array, axis, [(0, 1), (1, 0)])


def project_kernel(lengths_ref, *refs):
    sources, (out_ref, q_ref, k_ref, v_ref, residual_ref, weight_ref, arrived) = refs[:5], refs[5:]
    chunks = weight_ref.shape[0]
    depth = weight_ref.shape[1]
    copies = [
        pltpu.make_async_copy(source, held, arrived.at[i])
        for i, (source, held) in enumerate(
            zip(sources[:4], (q_ref, k_ref, v_ref, residual_ref), strict=True)
        )
    ] + [
        pltpu.make_async_copy(
            sources[4].at[pl.ds(i * depth, depth)], weight_ref.at[i], arrived.at[4 + i]
        )
        for i in range(chunks)
    ]
    for copy in copies:
        copy.start()
    count = lengths_ref.shape[0]
    tokens = count * SEQ
    pair_heads = k_ref.shape[1] // HEAD_DIM
    shared = q_ref.shape[1] // HEAD_DIM // pair_heads
    rows = shared * count

    def last_of(query):
        place = jnp.zeros_like(query)
        for b in range(count):
            place = jnp.where(query == b, b * SEQ + lengths_ref[b] - 1, place)
        return place

    def one_hot(hit):
        return jnp.where(hit, 1.0, 0.0).astype(jnp.bfloat16)

    row = lax.broadcasted_iota(jnp.int32, (rows, tokens), 0)
    token = lax.broadcasted_iota(jnp.int32, (rows, tokens), 1)
    query = row % count
    last = last_of(query)
    allowed = (token >= query * SEQ) & (token <= last)
    picks = [one_hot((token == last) & (row // count == h)) for h in range(shared)]
    for copy in copies[:3]:
        copy.wait()
    total = out_ref.shape[0]
    slot = lax.broadcasted_iota(jnp.int32, (total, rows), 0)
    source_row = lax.broadcasted_iota(jnp.int32, (total, rows), 1)
    spread = [one_hot(source_row == h * count + slot % count) for h in range(shared)]
    parts = []
    for g in range(pair_heads):
        columns = pl.ds(g * HEAD_DIM, HEAD_DIM)
        queries = sum(
            jnp.dot(
                picks[h],
                q_ref[:, pl.ds((g * shared + h) * HEAD_DIM, HEAD_DIM)],
                preferred_element_type=jnp.float32,
            )
            for h in range(shared)
        ).astype(jnp.bfloat16)
        logits = lax.dot_general(
            queries, k_ref[:, columns], (((1,), (1,)), ((), ())), preferred_element_type=jnp.float32
        ) / math.sqrt(HEAD_DIM)
        logits = jnp.where(allowed, logits, -1e30)
        weights = jnp.where(
            allowed, jnp.exp(logits - jnp.max(logits, axis=1, keepdims=True)), 0.0
        )
        attention = (weights / jnp.sum(weights, axis=1, keepdims=True)).astype(jnp.bfloat16)
        context = jnp.dot(
            attention, v_ref[:, columns], preferred_element_type=jnp.float32
        ).astype(jnp.bfloat16)
        parts += [
            jnp.dot(spread[h], context, preferred_element_type=jnp.float32).astype(jnp.bfloat16)
            for h in range(shared)
        ]
    place = lax.broadcasted_iota(jnp.int32, (total, tokens), 1)
    owner = lax.broadcasted_iota(jnp.int32, (total, tokens), 0) % count
    first = lax.axis_index(XL) + lax.axis_index(C) == 0
    copies[3].wait()
    terms = jnp.dot(
        one_hot((place == last_of(owner)) & first),
        residual_ref[...],
        preferred_element_type=jnp.float32,
    )
    per = depth // HEAD_DIM
    for i in range(chunks):
        part = jnp.concatenate(parts[i * per : (i + 1) * per], axis=1)
        copies[4 + i].wait()
        terms = terms + jnp.dot(part, weight_ref[i], preferred_element_type=jnp.float32)
    out_ref[...] = terms


def project(q_states, k_states, v_states, residual, out_weight, lengths, total):
    depth, width = out_weight.shape
    chunks = 4
    whole = [q_states, k_states, v_states, residual]
    arrays = [pltpu.with_memory_space_constraint(x, pltpu.HBM) for x in (*whole, out_weight)]
    return pl.pallas_call(
        project_kernel,
        name="project",
        out_shape=jax.ShapeDtypeStruct((total, width), jnp.float32),
        in_specs=[pl.BlockSpec(memory_space=pltpu.SMEM)]
        + [pl.BlockSpec(memory_space=pltpu.HBM)] * 5,
        out_specs=pl.BlockSpec(memory_space=pltpu.VMEM),
        scratch_shapes=[pltpu.VMEM(x.shape, x.dtype) for x in whole]
        + [
            pltpu.VMEM((chunks, depth // chunks, width), out_weight.dtype),
            pltpu.SemaphoreType.DMA((4 + chunks,)),
        ],
        compiler_params=pltpu.CompilerParams(vmem_limit_bytes=24 * 1024 * 1024),
    )(lengths, *arrays)


def embed_kernel(terms_ref, gain_ref, out_ref):
    groups = out_ref.shape[1]
    per = terms_ref.shape[0] // groups
    rows = []
    for g in range(groups):
        pooled = terms_ref[g * per]
        for t in range(1, per):
            pooled = pooled + terms_ref[g * per + t]
        scaled = pooled * gain_ref[...]
        magnitude = jnp.maximum(jnp.sqrt(jnp.sum(scaled * scaled, axis=1, keepdims=True)), 1.0)
        rows.append(scaled / magnitude)
    embed = jnp.concatenate(rows, axis=0).astype(jnp.bfloat16)
    for slot in range(out_ref.shape[0]):
        out_ref[slot] = embed


def embed_rows(terms, final_gain, groups, copies):
    width = terms.shape[-1]
    space = pl.BlockSpec(memory_space=pltpu.VMEM)
    return pl.pallas_call(
        embed_kernel,
        name="embed_rows",
        out_shape=jax.ShapeDtypeStruct((copies, groups, width), jnp.bfloat16),
        in_specs=[space] * 2,
        out_specs=space,
        compiler_params=pltpu.CompilerParams(vmem_limit_bytes=8 * 1024 * 1024),
    )(terms, final_gain.reshape(1, width))


def merge(peaks, totals, axes):
    peak = jnp.max(peaks, axis=axes, keepdims=True)
    total = jnp.sum(totals * jnp.exp(peaks - peak), axis=axes)
    return jnp.squeeze(peak, axes), total


def score_kernel(*refs):
    parts, blocks, (kept_ref, crossing_ref, stats_ref, rows) = refs[:4], refs[4:8], refs[8:]
    outs = [kept_ref.at[0], kept_ref.at[1], crossing_ref.at[0], crossing_ref.at[1]]
    me = lax.axis_index(YL) * 2 + lax.axis_index(ZL)
    for flip, part in enumerate(parts):
        rows[me ^ flip] = part[...]
    count = rows.shape[0] * rows.shape[1]
    peak = None
    for block, out in zip(blocks, outs, strict=True):
        scores = (
            lax.dot_general(
                rows[...].reshape(count, rows.shape[2]),
                block[...],
                (((1,), (1,)), ((), ())),
                preferred_element_type=jnp.float32,
            )
            * score_scale
        )
        out[...] = scores
        top = jnp.max(scores, axis=1, keepdims=True)
        peak = top if peak is None else jnp.maximum(peak, top)
    total = sum(jnp.sum(jnp.exp(out[...] - peak), axis=1, keepdims=True) for out in outs)
    lane = lax.broadcasted_iota(jnp.int32, (count, 128), 1)
    stats = jnp.transpose(jnp.where(lane == 0, peak, total))[:2]
    stats_ref[...] = jnp.broadcast_to(stats[None], stats_ref.shape)


def hold_kernel(*refs):
    count = len(refs) // 2
    sources, outs, arrived = refs[:count], refs[count : 2 * count], refs[-1]
    copies = [
        pltpu.make_async_copy(source, out, arrived.at[i])
        for i, (source, out) in enumerate(zip(sources, outs, strict=True))
    ]
    for copy in copies:
        copy.start()
    for copy in copies:
        copy.wait()


def hold(blocks):
    count = len(blocks)
    return pl.pallas_call(
        hold_kernel,
        name="hold",
        out_shape=[pltpu.VMEM(block.shape, block.dtype) for block in blocks],
        in_specs=[pl.BlockSpec(memory_space=pltpu.HBM)] * count,
        out_specs=[pl.BlockSpec(memory_space=pltpu.VMEM)] * count,
        scratch_shapes=[pltpu.SemaphoreType.DMA((count,))],
        cost_estimate=pl.CostEstimate(
            flops=1, bytes_accessed=4 * sum(b.size for b in blocks), transcendentals=0
        ),
        compiler_params=pltpu.CompilerParams(vmem_limit_bytes=12 * 1024 * 1024),
    )(*[pltpu.with_memory_space_constraint(block, pltpu.HBM) for block in blocks])


def score_blocks(parts, blocks, copies):
    each, width = parts[0].shape
    count = len(parts) * each
    passages = blocks[0].shape[0]
    space = pl.BlockSpec(memory_space=pltpu.VMEM)
    blocks = [pltpu.with_memory_space_constraint(block, pltpu.VMEM) for block in blocks]
    return pl.pallas_call(
        score_kernel,
        name="score_blocks",
        out_shape=[jax.ShapeDtypeStruct((2, count, passages), jnp.float32)] * 2
        + [jax.ShapeDtypeStruct((copies, 2, count), jnp.float32)],
        in_specs=[space] * 8,
        out_specs=[space] * 3,
        scratch_shapes=[pltpu.VMEM((len(parts), each, width), jnp.bfloat16)],
        cost_estimate=pl.CostEstimate(
            flops=8 * count * passages * width,
            bytes_accessed=8 * passages * width,
            transcendentals=4 * count * passages,
        ),
        compiler_params=pltpu.CompilerParams(vmem_limit_bytes=16 * 1024 * 1024),
    )(*parts, *blocks)


def arrange_kernel(sizes, kept_ref, crossed_ref, given_ref, out_ref, by_owner, placed):
    xh, yh, yl, zh, zl, tensor = sizes
    me = lax.axis_index(XL) * 2 + lax.axis_index(C)
    for flip, ref in enumerate(
        (kept_ref.at[0], given_ref.at[0], crossed_ref.at[0], given_ref.at[1])
    ):
        for half in range(placed.shape[0]):
            by_owner[me ^ flip, half] = ref[:, pl.ds(half * 128, 128)]
    for t in range(tensor):
        for near in range(yl * zl):
            y0, z0 = near // zl, near % zl
            for y1 in range(yh):
                for x in range(xh):
                    start = (near * yh + y1) * zh * xh + x
                    to = ((x * yh + y1) * yl + y0) * zh * zl + z0
                    for half in range(placed.shape[0]):
                        placed[half, pl.ds(to * tensor + t, zh, stride=zl * tensor)] = by_owner[
                            t, half, pl.ds(start, zh, stride=xh)
                        ]
    for half in range(placed.shape[0]):
        out_ref[:, pl.ds(half * 128, 128)] = placed[half]


def arrange(kept, crossed, given, sizes):
    _, rows, passages = kept.shape
    tensor = sizes[-1]
    space = pl.BlockSpec(memory_space=pltpu.VMEM)
    return pl.pallas_call(
        functools.partial(arrange_kernel, sizes),
        name="arrange",
        out_shape=jax.ShapeDtypeStruct((rows * tensor, passages), jnp.float32),
        in_specs=[space] * 3,
        out_specs=space,
        scratch_shapes=[
            pltpu.VMEM((tensor, passages // 128, rows, 128), jnp.float32),
            pltpu.VMEM((passages // 128, rows * tensor, 128), jnp.float32),
        ],
        compiler_params=pltpu.CompilerParams(vmem_limit_bytes=8 * 1024 * 1024),
    )(kept, crossed, given)


def step(q_states, k_states, v_states, residual, out_weight, final_gain, passages, lengths):
    xh, yh, yl, zh, zl, xl, c = (lax.axis_size(axis) for axis in CORPUS_TENSOR)
    tensor = xl * c
    width = out_weight.shape[1]
    rows = yh * yl * zh * zl * xh
    terms = project(q_states, k_states, v_states, residual, out_weight, lengths, xh * tensor)

    terms = lax.all_to_all(
        terms.reshape(xh * tensor, 1, width), (XH, XL, C), 0, 0, tiled=True
    )

    across = swap(passages, XL)
    partner = swap(passages, C)
    both = swap(across, C)

    embed = embed_rows(terms, final_gain, xh, yh * zh)
    gathered = lax.all_to_all(embed, (YH, ZH), 0, 0, tiled=True).reshape(-1, width)
    shift = functools.partial(shifted, gathered)
    near_both = shift((YH, YL, ZH, ZL), 1, 1)
    near_y = shift((YH, YL, ZH, ZL), -1, 0)
    near_z = shift((YH, YL, ZH, ZL), 0, -1)

    held = hold((passages, partner, across))

    kept, crossing, stats = score_blocks(
        (gathered, near_z, near_y, near_both), (*held, both), zh * zl * c
    )

    crossed = swap(crossing, XL)
    given = swap(jnp.stack([kept[1], crossed[1]]), C)
    scores = arrange(kept, crossed, given, (xh, yh, yl, zh, zl, tensor))

    pairs = lax.all_to_all(stats, (ZH, ZL, C), 0, 0, tiled=True)
    pairs = pairs.reshape(zh * zl, c, 2, rows)
    peak, total = merge(pairs[:, :, 0], pairs[:, :, 1], 0)
    pairs = to_all(jnp.stack([peak, total]), (XH, YH, YL, XL))
    pairs = pairs.reshape(xh * yh * yl, xl, 2, c, rows)
    peak, total = merge(pairs[:, :, 0], pairs[:, :, 1], 0)
    log_norm = (peak + jnp.log(total)).reshape(tensor, rows)

    log_norm = log_norm.reshape(tensor, yl, zl, yh, zh, xh).transpose(5, 3, 1, 4, 2, 0)
    return scores, log_norm.reshape(rows * tensor)


def solution(mesh):
    split = Mesh(mesh.devices.reshape(2, 4, 2, 6, 2, 2, 2), CORPUS_TENSOR)
    in_specs = (
        P(CORPUS, TENSOR),
        P(CORPUS, TENSOR),
        P(CORPUS, TENSOR),
        P(CORPUS, None),
        P(TENSOR, None),
        P(),
        P(CORPUS_TENSOR, None),
        P(CORPUS),
    )
    out_specs = (P(None, CORPUS_TENSOR), P())
    return jax.shard_map(step, mesh=split, in_specs=in_specs, out_specs=out_specs, check_vma=False)
```

```python
import functools
import math

import jax
import jax.numpy as jnp
from jax import lax
from jax.experimental import pallas as pl
from jax.experimental.pallas import tpu as pltpu
from jax.sharding import Mesh
from jax.sharding import PartitionSpec as P


HEAD_DIM = 128
SEQ = 16
XH, YH, YL, ZH, ZL, XL, C = "xh", "yh", "yl", "zh", "zl", "xl", "c"
TENSOR = (XL, C)
CORPUS = (XH, YH, YL, ZH, ZL)
CORPUS_TENSOR = (*CORPUS, *TENSOR)

score_scale = 50.0


def size_of(axes):
    return math.prod(lax.axis_size(axis) for axis in axes)


def finish_kernel(sizes, pairs_ref, out_ref):
    xh, yh, yl, zh, zl, xl, c = sizes
    members, count = pairs_ref.shape[0] // xl, pairs_ref.shape[-1]
    row = lax.broadcasted_iota(jnp.int32, (count, out_ref.shape[0]), 0)
    x, z1, y1 = row % xh, row // xh % zh, row // (xh * zh) % yh
    z0, y0 = row // (xh * zh * yh) % zl, row // (xh * zh * yh * zl)
    place = (((x * yh + y1) * yl + y0) * zh + z1) * zl + z0
    target = lax.broadcasted_iota(jnp.int32, row.shape, 1)
    out = jnp.zeros((1, out_ref.shape[0]), jnp.float32)
    for t in range(xl * c):
        peak, total = merged([pairs_ref[m * xl + t // c, t % c] for m in range(members)])
        value = peak + jnp.log(total)
        high = value.astype(jnp.bfloat16)
        rest = value - high.astype(jnp.float32)
        middle = rest.astype(jnp.bfloat16)
        low = (rest - middle.astype(jnp.float32)).astype(jnp.bfloat16)
        chosen = jnp.where(place * (xl * c) + t == target, 1.0, 0.0).astype(jnp.bfloat16)
        for term in (low, middle, high):
            spread = jnp.broadcast_to(term.astype(jnp.float32), (8, count)).astype(jnp.bfloat16)
            out = out + jnp.dot(spread, chosen, preferred_element_type=jnp.float32)[:1]
    out_ref[...] = out[0]


def finish(pairs, sizes):
    space = pl.BlockSpec(memory_space=pltpu.VMEM)
    queries = pairs.shape[-1] * sizes[-1] * sizes[-2]
    return pl.pallas_call(
        functools.partial(finish_kernel, sizes),
        name="finish",
        out_shape=jax.ShapeDtypeStruct((queries,), jnp.float32),
        in_specs=[space],
        out_specs=space,
        compiler_params=pltpu.CompilerParams(vmem_limit_bytes=8 * 1024 * 1024),
    )(pairs)


def shifted(array, axes, along_y, along_z):
    y, z = size_of(axes[:2]), size_of(axes[2:])
    moves = [
        (i * z + j, (i + along_y) % y * z + (j + along_z) % z) for i in range(y) for j in range(z)
    ]
    return lax.ppermute(array, axes, moves)


def swap(array, axis):
    return lax.ppermute(array, axis, [(0, 1), (1, 0)])


def project_kernel(*refs):
    sources, lengths, refs = refs[:5], refs[5], refs[6:]
    out_ref, q_ref, k_ref, v_ref, residual_ref, weight_ref, lengths_ref, arrived, known = refs
    counted = pltpu.make_async_copy(lengths, lengths_ref, known)
    counted.start()
    chunks = weight_ref.shape[0]
    depth = weight_ref.shape[1]
    copies = [
        pltpu.make_async_copy(source, held, arrived.at[i])
        for i, (source, held) in enumerate(
            zip(sources[:4], (q_ref, k_ref, v_ref, residual_ref), strict=True)
        )
    ] + [
        pltpu.make_async_copy(
            sources[4].at[pl.ds(i * depth, depth)], weight_ref.at[i], arrived.at[4 + i]
        )
        for i in range(chunks)
    ]
    for copy in copies:
        copy.start()
    counted.wait()
    count = lengths_ref.shape[0]
    tokens = count * SEQ
    pair_heads = k_ref.shape[1] // HEAD_DIM
    shared = q_ref.shape[1] // HEAD_DIM // pair_heads
    rows = shared * count

    def last_of(query):
        place = jnp.zeros_like(query)
        for b in range(count):
            place = jnp.where(query == b, b * SEQ + lengths_ref[b] - 1, place)
        return place

    def one_hot(hit):
        return jnp.where(hit, 1.0, 0.0).astype(jnp.bfloat16)

    row = lax.broadcasted_iota(jnp.int32, (rows, tokens), 0)
    token = lax.broadcasted_iota(jnp.int32, (rows, tokens), 1)
    query = row % count
    last = last_of(query)
    allowed = (token >= query * SEQ) & (token <= last)
    picks = [one_hot((token == last) & (row // count == h)) for h in range(shared)]
    for copy in copies[:3]:
        copy.wait()
    total = out_ref.shape[0]
    slot = lax.broadcasted_iota(jnp.int32, (total, rows), 0)
    source_row = lax.broadcasted_iota(jnp.int32, (total, rows), 1)
    spread = [one_hot(source_row == h * count + slot % count) for h in range(shared)]
    parts = []
    for g in range(pair_heads):
        columns = pl.ds(g * HEAD_DIM, HEAD_DIM)
        queries = sum(
            jnp.dot(
                picks[h],
                q_ref[:, pl.ds((g * shared + h) * HEAD_DIM, HEAD_DIM)],
                preferred_element_type=jnp.float32,
            )
            for h in range(shared)
        ).astype(jnp.bfloat16)
        logits = lax.dot_general(
            queries, k_ref[:, columns], (((1,), (1,)), ((), ())), preferred_element_type=jnp.float32
        ) / math.sqrt(HEAD_DIM)
        logits = jnp.where(allowed, logits, -1e30)
        weights = jnp.where(
            allowed, jnp.exp(logits - jnp.max(logits, axis=1, keepdims=True)), 0.0
        )
        attention = (weights / jnp.sum(weights, axis=1, keepdims=True)).astype(jnp.bfloat16)
        context = jnp.dot(
            attention, v_ref[:, columns], preferred_element_type=jnp.float32
        ).astype(jnp.bfloat16)
        parts += [
            jnp.dot(spread[h], context, preferred_element_type=jnp.float32).astype(jnp.bfloat16)
            for h in range(shared)
        ]
    place = lax.broadcasted_iota(jnp.int32, (total, tokens), 1)
    owner = lax.broadcasted_iota(jnp.int32, (total, tokens), 0) % count
    first = lax.axis_index(XL) + lax.axis_index(C) == 0
    copies[3].wait()
    terms = jnp.dot(
        one_hot((place == last_of(owner)) & first),
        residual_ref[...],
        preferred_element_type=jnp.float32,
    )
    per = depth // HEAD_DIM
    for i in range(chunks):
        part = jnp.concatenate(parts[i * per : (i + 1) * per], axis=1)
        copies[4 + i].wait()
        terms = terms + jnp.dot(part, weight_ref[i], preferred_element_type=jnp.float32)
    for d in range(total):
        out_ref[d] = terms[d : d + 1]


def project(q_states, k_states, v_states, residual, out_weight, lengths, total):
    depth, width = out_weight.shape
    chunks = 4
    whole = [q_states, k_states, v_states, residual]
    arrays = [
        pltpu.with_memory_space_constraint(x, pltpu.HBM) for x in (*whole, out_weight, lengths)
    ]
    return pl.pallas_call(
        project_kernel,
        name="project",
        out_shape=jax.ShapeDtypeStruct((total, 1, width), jnp.float32),
        in_specs=[pl.BlockSpec(memory_space=pltpu.HBM)] * 6,
        out_specs=pl.BlockSpec(memory_space=pltpu.VMEM),
        scratch_shapes=[pltpu.VMEM(x.shape, x.dtype) for x in whole]
        + [
            pltpu.VMEM((chunks, depth // chunks, width), out_weight.dtype),
            pltpu.SMEM(lengths.shape, lengths.dtype),
            pltpu.SemaphoreType.DMA((4 + chunks,)),
            pltpu.SemaphoreType.DMA,
        ],
        compiler_params=pltpu.CompilerParams(vmem_limit_bytes=24 * 1024 * 1024),
    )(*arrays)


def embed_kernel(terms_ref, gain_ref, out_ref):
    groups = out_ref.shape[1]
    per = terms_ref.shape[0] // groups
    rows = []
    for g in range(groups):
        pooled = terms_ref[g * per]
        for t in range(1, per):
            pooled = pooled + terms_ref[g * per + t]
        scaled = pooled * gain_ref[...]
        magnitude = jnp.maximum(jnp.sqrt(jnp.sum(scaled * scaled, axis=1, keepdims=True)), 1.0)
        rows.append(scaled / magnitude)
    embed = jnp.concatenate(rows, axis=0).astype(jnp.bfloat16)
    for slot in range(out_ref.shape[0]):
        out_ref[slot] = embed


def embed_rows(terms, final_gain, groups, copies):
    width = terms.shape[-1]
    space = pl.BlockSpec(memory_space=pltpu.VMEM)
    return pl.pallas_call(
        embed_kernel,
        name="embed_rows",
        out_shape=jax.ShapeDtypeStruct((copies, groups, width), jnp.bfloat16),
        in_specs=[space] * 2,
        out_specs=space,
        compiler_params=pltpu.CompilerParams(vmem_limit_bytes=8 * 1024 * 1024),
    )(terms, final_gain.reshape(1, width))


def merged(rows):
    peaks = [row[:1] for row in rows]
    peak = functools.reduce(jnp.maximum, peaks)
    return peak, sum(row[1:] * jnp.exp(p - peak) for row, p in zip(rows, peaks, strict=True))


def merge_kernel(group, pairs_ref, out_ref):
    members = pairs_ref.shape[0] // group
    parts = [
        jnp.concatenate(merged([pairs_ref[m * group + part] for m in range(members)]), axis=0)
        for part in range(group)
    ]
    for slot in range(out_ref.shape[0]):
        for part in range(group):
            out_ref[slot, part] = parts[part]


def merge(pairs, group, copies):
    space = pl.BlockSpec(memory_space=pltpu.VMEM)
    return pl.pallas_call(
        functools.partial(merge_kernel, group),
        name="merge",
        out_shape=jax.ShapeDtypeStruct((copies, group, *pairs.shape[1:]), jnp.float32),
        in_specs=[space],
        out_specs=space,
        compiler_params=pltpu.CompilerParams(vmem_limit_bytes=8 * 1024 * 1024),
    )(pairs)


def score_kernel(*refs):
    parts, blocks, (kept_ref, crossing_ref, stats_ref, rows) = refs[:4], refs[4:8], refs[8:]
    outs = [kept_ref.at[0], kept_ref.at[1], crossing_ref.at[0], crossing_ref.at[1]]
    me = lax.axis_index(YL) * 2 + lax.axis_index(ZL)
    for flip, part in enumerate(parts):
        rows[me ^ flip] = part[...]
    count = rows.shape[0] * rows.shape[1]
    peak = None
    for block, out in zip(blocks, outs, strict=True):
        scores = (
            lax.dot_general(
                rows[...].reshape(count, rows.shape[2]),
                block[...],
                (((1,), (1,)), ((), ())),
                preferred_element_type=jnp.float32,
            )
            * score_scale
        )
        out[...] = scores
        top = jnp.max(scores, axis=1, keepdims=True)
        peak = top if peak is None else jnp.maximum(peak, top)
    total = sum(jnp.sum(jnp.exp(out[...] - peak), axis=1, keepdims=True) for out in outs)
    lane = lax.broadcasted_iota(jnp.int32, (count, 128), 1)
    stats = jnp.transpose(jnp.where(lane == 0, peak, total))[:2]
    stats_ref[...] = jnp.broadcast_to(stats[None], stats_ref.shape)


def hold_kernel(*refs):
    count = len(refs) // 2
    sources, outs, arrived = refs[:count], refs[count : 2 * count], refs[-1]
    copies = [
        pltpu.make_async_copy(source, out, arrived.at[i])
        for i, (source, out) in enumerate(zip(sources, outs, strict=True))
    ]
    for copy in copies:
        copy.start()
    for copy in copies:
        copy.wait()


def hold(blocks):
    count = len(blocks)
    return pl.pallas_call(
        hold_kernel,
        name="hold",
        out_shape=[pltpu.VMEM(block.shape, block.dtype) for block in blocks],
        in_specs=[pl.BlockSpec(memory_space=pltpu.HBM)] * count,
        out_specs=[pl.BlockSpec(memory_space=pltpu.VMEM)] * count,
        scratch_shapes=[pltpu.SemaphoreType.DMA((count,))],
        cost_estimate=pl.CostEstimate(
            flops=1, bytes_accessed=4 * sum(b.size for b in blocks), transcendentals=0
        ),
        compiler_params=pltpu.CompilerParams(vmem_limit_bytes=12 * 1024 * 1024),
    )(*[pltpu.with_memory_space_constraint(block, pltpu.HBM) for block in blocks])


def score_blocks(parts, blocks, copies):
    each, width = parts[0].shape
    count = len(parts) * each
    passages = blocks[0].shape[0]
    space = pl.BlockSpec(memory_space=pltpu.VMEM)
    blocks = [pltpu.with_memory_space_constraint(block, pltpu.VMEM) for block in blocks]
    return pl.pallas_call(
        score_kernel,
        name="score_blocks",
        out_shape=[jax.ShapeDtypeStruct((2, count, passages), jnp.float32)] * 2
        + [jax.ShapeDtypeStruct((copies, 2, count), jnp.float32)],
        in_specs=[space] * 8,
        out_specs=[space] * 3,
        scratch_shapes=[pltpu.VMEM((len(parts), each, width), jnp.bfloat16)],
        cost_estimate=pl.CostEstimate(
            flops=8 * count * passages * width,
            bytes_accessed=8 * passages * width,
            transcendentals=4 * count * passages,
        ),
        compiler_params=pltpu.CompilerParams(vmem_limit_bytes=16 * 1024 * 1024),
    )(*parts, *blocks)


def arrange_kernel(sizes, kept_ref, crossed_ref, given_ref, out_ref, by_owner, placed):
    xh, yh, yl, zh, zl, tensor = sizes
    me = lax.axis_index(XL) * 2 + lax.axis_index(C)
    for flip, ref in enumerate(
        (kept_ref.at[0], given_ref.at[0], crossed_ref.at[0], given_ref.at[1])
    ):
        for half in range(placed.shape[0]):
            by_owner[me ^ flip, half] = ref[:, pl.ds(half * 128, 128)]
    for t in range(tensor):
        for near in range(yl * zl):
            y0, z0 = near // zl, near % zl
            for y1 in range(yh):
                for x in range(xh):
                    start = (near * yh + y1) * zh * xh + x
                    to = ((x * yh + y1) * yl + y0) * zh * zl + z0
                    for half in range(placed.shape[0]):
                        placed[half, pl.ds(to * tensor + t, zh, stride=zl * tensor)] = by_owner[
                            t, half, pl.ds(start, zh, stride=xh)
                        ]
    for half in range(placed.shape[0]):
        out_ref[:, pl.ds(half * 128, 128)] = placed[half]


def arrange(kept, crossed, given, sizes):
    _, rows, passages = kept.shape
    tensor = sizes[-1]
    space = pl.BlockSpec(memory_space=pltpu.VMEM)
    return pl.pallas_call(
        functools.partial(arrange_kernel, sizes),
        name="arrange",
        out_shape=jax.ShapeDtypeStruct((rows * tensor, passages), jnp.float32),
        in_specs=[space] * 3,
        out_specs=space,
        scratch_shapes=[
            pltpu.VMEM((tensor, passages // 128, rows, 128), jnp.float32),
            pltpu.VMEM((passages // 128, rows * tensor, 128), jnp.float32),
        ],
        compiler_params=pltpu.CompilerParams(vmem_limit_bytes=8 * 1024 * 1024),
    )(kept, crossed, given)


def step(q_states, k_states, v_states, residual, out_weight, final_gain, passages, lengths):
    xh, yh, yl, zh, zl, xl, c = (lax.axis_size(axis) for axis in CORPUS_TENSOR)
    tensor = xl * c
    width = out_weight.shape[1]
    terms = project(q_states, k_states, v_states, residual, out_weight, lengths, xh * tensor)

    terms = lax.all_to_all(terms, (XH, XL, C), 0, 0, tiled=True)

    across = swap(passages, XL)
    partner = swap(passages, C)
    both = swap(across, C)

    embed = embed_rows(terms, final_gain, xh, yh * zh)
    gathered = lax.all_to_all(embed, (YH, ZH), 0, 0, tiled=True).reshape(-1, width)
    shift = functools.partial(shifted, gathered)
    near_both = shift((YH, YL, ZH, ZL), 1, 1)
    near_y = shift((YH, YL, ZH, ZL), -1, 0)
    near_z = shift((YH, YL, ZH, ZL), 0, -1)

    held = hold((passages, partner, across))

    kept, crossing, stats = score_blocks(
        (gathered, near_z, near_y, near_both), (*held, both), zh * zl * c
    )

    crossed = swap(crossing, XL)
    given = swap(jnp.stack([kept[1], crossed[1]]), C)
    scores = arrange(kept, crossed, given, (xh, yh, yl, zh, zl, tensor))

    pairs = lax.all_to_all(stats, (ZH, ZL, C), 0, 0, tiled=True)
    pairs = lax.all_to_all(merge(pairs, c, xh * yh * yl * xl), (XH, YH, YL, XL), 0, 0, tiled=True)
    return scores, finish(pairs, (xh, yh, yl, zh, zl, xl, c))


def solution(mesh):
    split = Mesh(mesh.devices.reshape(2, 4, 2, 6, 2, 2, 2), CORPUS_TENSOR)
    in_specs = (
        P(CORPUS, TENSOR),
        P(CORPUS, TENSOR),
        P(CORPUS, TENSOR),
        P(CORPUS, None),
        P(TENSOR, None),
        P(),
        P(CORPUS_TENSOR, None),
        P(CORPUS),
    )
    out_specs = (P(None, CORPUS_TENSOR), P())
    return jax.shard_map(step, mesh=split, in_specs=in_specs, out_specs=out_specs, check_vma=False)
```

```python
import functools
import math

import jax
import jax.numpy as jnp
from jax import lax
from jax.experimental import pallas as pl
from jax.experimental.pallas import tpu as pltpu
from jax.sharding import Mesh
from jax.sharding import PartitionSpec as P


HEAD_DIM = 128
SEQ = 16
XH, YH, YL, ZH, ZL, XL, C = "xh", "yh", "yl", "zh", "zl", "xl", "c"
TENSOR = (XL, C)
CORPUS = (XH, YH, YL, ZH, ZL)
CORPUS_TENSOR = (*CORPUS, *TENSOR)

score_scale = 50.0


def size_of(axes):
    return math.prod(lax.axis_size(axis) for axis in axes)


def finish_kernel(sizes, pairs_ref, out_ref):
    xh, yh, yl, zh, zl, xl, c = sizes
    members, count = pairs_ref.shape[0] // xl, pairs_ref.shape[-1]
    row = lax.broadcasted_iota(jnp.int32, (count, 1), 0)
    x, z1, y1 = row % xh, row // xh % zh, row // (xh * zh) % yh
    z0, y0 = row // (xh * zh * yh) % zl, row // (xh * zh * yh * zl)
    place = ((((x * yh + y1) * yl + y0) * zh + z1) * zl + z0) * (xl * c)
    target = lax.broadcasted_iota(jnp.int32, (count, out_ref.shape[0]), 1)
    term = lax.broadcasted_iota(jnp.int32, (8, count), 0)
    out = jnp.zeros((8, out_ref.shape[0]), jnp.float32)
    for t in range(xl * c):
        peak, total = merged([pairs_ref[m * xl + t // c, t % c] for m in range(members)])
        value = peak + jnp.log(total)
        high = value.astype(jnp.bfloat16).astype(jnp.float32)
        middle = (value - high).astype(jnp.bfloat16).astype(jnp.float32)
        low = value - high - middle
        terms = jnp.where(term == 0, high, jnp.where(term == 1, middle, low))
        terms = jnp.where(term < 3, terms, 0.0).astype(jnp.bfloat16)
        chosen = jnp.where(place + t == target, 1.0, 0.0).astype(jnp.bfloat16)
        out = out + jnp.dot(terms, chosen, preferred_element_type=jnp.float32)
    out = (out[2:3] + out[1:2]) + out[0:1]
    out_ref[...] = out[0]


def finish(pairs, sizes):
    space = pl.BlockSpec(memory_space=pltpu.VMEM)
    queries = pairs.shape[-1] * sizes[-1] * sizes[-2]
    return pl.pallas_call(
        functools.partial(finish_kernel, sizes),
        name="finish",
        out_shape=jax.ShapeDtypeStruct((queries,), jnp.float32),
        in_specs=[space],
        out_specs=space,
        compiler_params=pltpu.CompilerParams(vmem_limit_bytes=8 * 1024 * 1024),
    )(pairs)


def shifted(array, axes, along_y, along_z):
    y, z = size_of(axes[:2]), size_of(axes[2:])
    moves = [
        (i * z + j, (i + along_y) % y * z + (j + along_z) % z) for i in range(y) for j in range(z)
    ]
    return lax.ppermute(array, axes, moves)


def swap(array, axis):
    return lax.ppermute(array, axis, [(0, 1), (1, 0)])


def project_kernel(*refs):
    sources, lengths, refs = refs[:5], refs[5], refs[6:]
    out_ref, q_ref, k_ref, v_ref, residual_ref, weight_ref, lengths_ref, arrived, known = refs
    counted = pltpu.make_async_copy(lengths, lengths_ref, known)
    counted.start()
    chunks = weight_ref.shape[0]
    depth = weight_ref.shape[1]
    copies = [
        pltpu.make_async_copy(source, held, arrived.at[i])
        for i, (source, held) in enumerate(
            zip(sources[:4], (q_ref, k_ref, v_ref, residual_ref), strict=True)
        )
    ] + [
        pltpu.make_async_copy(
            sources[4].at[pl.ds(i * depth, depth)], weight_ref.at[i], arrived.at[4 + i]
        )
        for i in range(chunks)
    ]
    for copy in copies:
        copy.start()
    counted.wait()
    count = lengths_ref.shape[0]
    tokens = count * SEQ
    pair_heads = k_ref.shape[1] // HEAD_DIM
    shared = q_ref.shape[1] // HEAD_DIM // pair_heads
    rows = shared * count

    def last_of(query):
        place = jnp.zeros_like(query)
        for b in range(count):
            place = jnp.where(query == b, b * SEQ + lengths_ref[b] - 1, place)
        return place

    def one_hot(hit):
        return jnp.where(hit, 1.0, 0.0).astype(jnp.bfloat16)

    row = lax.broadcasted_iota(jnp.int32, (rows, tokens), 0)
    token = lax.broadcasted_iota(jnp.int32, (rows, tokens), 1)
    query = row % count
    last = last_of(query)
    allowed = (token >= query * SEQ) & (token <= last)
    picks = [one_hot((token == last) & (row // count == h)) for h in range(shared)]
    for copy in copies[:3]:
        copy.wait()
    total = out_ref.shape[0]
    slot = lax.broadcasted_iota(jnp.int32, (total, rows), 0)
    source_row = lax.broadcasted_iota(jnp.int32, (total, rows), 1)
    spread = [one_hot(source_row == h * count + slot % count) for h in range(shared)]
    parts = []
    for g in range(pair_heads):
        columns = pl.ds(g * HEAD_DIM, HEAD_DIM)
        queries = sum(
            jnp.dot(
                picks[h],
                q_ref[:, pl.ds((g * shared + h) * HEAD_DIM, HEAD_DIM)],
                preferred_element_type=jnp.float32,
            )
            for h in range(shared)
        ).astype(jnp.bfloat16)
        logits = lax.dot_general(
            queries, k_ref[:, columns], (((1,), (1,)), ((), ())), preferred_element_type=jnp.float32
        ) / math.sqrt(HEAD_DIM)
        logits = jnp.where(allowed, logits, -1e30)
        weights = jnp.where(
            allowed, jnp.exp(logits - jnp.max(logits, axis=1, keepdims=True)), 0.0
        )
        attention = (weights / jnp.sum(weights, axis=1, keepdims=True)).astype(jnp.bfloat16)
        context = jnp.dot(
            attention, v_ref[:, columns], preferred_element_type=jnp.float32
        ).astype(jnp.bfloat16)
        parts += [
            jnp.dot(spread[h], context, preferred_element_type=jnp.float32).astype(jnp.bfloat16)
            for h in range(shared)
        ]
    place = lax.broadcasted_iota(jnp.int32, (total, tokens), 1)
    owner = lax.broadcasted_iota(jnp.int32, (total, tokens), 0) % count
    first = lax.axis_index(XL) + lax.axis_index(C) == 0
    copies[3].wait()
    terms = jnp.dot(
        one_hot((place == last_of(owner)) & first),
        residual_ref[...],
        preferred_element_type=jnp.float32,
    )
    per = depth // HEAD_DIM
    for i in range(chunks):
        part = jnp.concatenate(parts[i * per : (i + 1) * per], axis=1)
        copies[4 + i].wait()
        terms = terms + jnp.dot(part, weight_ref[i], preferred_element_type=jnp.float32)
    for d in range(total):
        out_ref[d] = terms[d : d + 1]


def project(q_states, k_states, v_states, residual, out_weight, lengths, total):
    depth, width = out_weight.shape
    chunks = 8
    whole = [q_states, k_states, v_states, residual]
    arrays = [
        pltpu.with_memory_space_constraint(x, pltpu.HBM) for x in (*whole, out_weight, lengths)
    ]
    return pl.pallas_call(
        project_kernel,
        name="project",
        out_shape=jax.ShapeDtypeStruct((total, 1, width), jnp.float32),
        in_specs=[pl.BlockSpec(memory_space=pltpu.HBM)] * 6,
        out_specs=pl.BlockSpec(memory_space=pltpu.VMEM),
        scratch_shapes=[pltpu.VMEM(x.shape, x.dtype) for x in whole]
        + [
            pltpu.VMEM((chunks, depth // chunks, width), out_weight.dtype),
            pltpu.SMEM(lengths.shape, lengths.dtype),
            pltpu.SemaphoreType.DMA((4 + chunks,)),
            pltpu.SemaphoreType.DMA,
        ],
        compiler_params=pltpu.CompilerParams(vmem_limit_bytes=24 * 1024 * 1024),
    )(*arrays)


def embed_kernel(terms_ref, gain_ref, out_ref):
    groups = out_ref.shape[1]
    per = terms_ref.shape[0] // groups
    rows = []
    for g in range(groups):
        pooled = terms_ref[g * per]
        for t in range(1, per):
            pooled = pooled + terms_ref[g * per + t]
        scaled = pooled * gain_ref[...]
        magnitude = jnp.maximum(jnp.sqrt(jnp.sum(scaled * scaled, axis=1, keepdims=True)), 1.0)
        rows.append(scaled / magnitude)
    embed = jnp.concatenate(rows, axis=0).astype(jnp.bfloat16)
    for slot in range(out_ref.shape[0]):
        out_ref[slot] = embed


def embed_rows(terms, final_gain, groups, copies):
    width = terms.shape[-1]
    space = pl.BlockSpec(memory_space=pltpu.VMEM)
    return pl.pallas_call(
        embed_kernel,
        name="embed_rows",
        out_shape=jax.ShapeDtypeStruct((copies, groups, width), jnp.bfloat16),
        in_specs=[space] * 2,
        out_specs=space,
        compiler_params=pltpu.CompilerParams(vmem_limit_bytes=8 * 1024 * 1024),
    )(terms, final_gain.reshape(1, width))


def merged(rows):
    peaks = [row[:1] for row in rows]
    peak = functools.reduce(jnp.maximum, peaks)
    return peak, sum(row[1:] * jnp.exp(p - peak) for row, p in zip(rows, peaks, strict=True))


def merge_kernel(group, pairs_ref, out_ref):
    members = pairs_ref.shape[0] // group
    parts = [
        jnp.concatenate(merged([pairs_ref[m * group + part] for m in range(members)]), axis=0)
        for part in range(group)
    ]
    for slot in range(out_ref.shape[0]):
        for part in range(group):
            out_ref[slot, part] = parts[part]


def merge(pairs, group, copies):
    space = pl.BlockSpec(memory_space=pltpu.VMEM)
    return pl.pallas_call(
        functools.partial(merge_kernel, group),
        name="merge",
        out_shape=jax.ShapeDtypeStruct((copies, group, *pairs.shape[1:]), jnp.float32),
        in_specs=[space],
        out_specs=space,
        compiler_params=pltpu.CompilerParams(vmem_limit_bytes=8 * 1024 * 1024),
    )(pairs)


def score_kernel(*refs):
    parts, blocks, (kept_ref, crossing_ref, stats_ref, rows) = refs[:4], refs[4:8], refs[8:]
    outs = [kept_ref.at[0], kept_ref.at[1], crossing_ref.at[0], crossing_ref.at[1]]
    me = lax.axis_index(YL) * 2 + lax.axis_index(ZL)
    for flip, part in enumerate(parts):
        rows[me ^ flip] = part[...]
    count = rows.shape[0] * rows.shape[1]
    peak = None
    for block, out in zip(blocks, outs, strict=True):
        scores = (
            lax.dot_general(
                rows[...].reshape(count, rows.shape[2]),
                block[...],
                (((1,), (1,)), ((), ())),
                preferred_element_type=jnp.float32,
            )
            * score_scale
        )
        out[...] = scores
        top = jnp.max(scores, axis=1, keepdims=True)
        peak = top if peak is None else jnp.maximum(peak, top)
    total = sum(jnp.sum(jnp.exp(out[...] - peak), axis=1, keepdims=True) for out in outs)
    lane = lax.broadcasted_iota(jnp.int32, (count, 128), 1)
    stats = jnp.transpose(jnp.where(lane == 0, peak, total))[:2]
    stats_ref[...] = jnp.broadcast_to(stats[None], stats_ref.shape)


def hold_kernel(*refs):
    count = len(refs) // 2
    sources, outs, arrived = refs[:count], refs[count : 2 * count], refs[-1]
    copies = [
        pltpu.make_async_copy(source, out, arrived.at[i])
        for i, (source, out) in enumerate(zip(sources, outs, strict=True))
    ]
    for copy in copies:
        copy.start()
    for copy in copies:
        copy.wait()


def hold(blocks):
    count = len(blocks)
    return pl.pallas_call(
        hold_kernel,
        name="hold",
        out_shape=[pltpu.VMEM(block.shape, block.dtype) for block in blocks],
        in_specs=[pl.BlockSpec(memory_space=pltpu.HBM)] * count,
        out_specs=[pl.BlockSpec(memory_space=pltpu.VMEM)] * count,
        scratch_shapes=[pltpu.SemaphoreType.DMA((count,))],
        cost_estimate=pl.CostEstimate(
            flops=1, bytes_accessed=4 * sum(b.size for b in blocks), transcendentals=0
        ),
        compiler_params=pltpu.CompilerParams(vmem_limit_bytes=12 * 1024 * 1024),
    )(*[pltpu.with_memory_space_constraint(block, pltpu.HBM) for block in blocks])


def score_blocks(parts, blocks, copies):
    each, width = parts[0].shape
    count = len(parts) * each
    passages = blocks[0].shape[0]
    space = pl.BlockSpec(memory_space=pltpu.VMEM)
    blocks = [pltpu.with_memory_space_constraint(block, pltpu.VMEM) for block in blocks]
    return pl.pallas_call(
        score_kernel,
        name="score_blocks",
        out_shape=[jax.ShapeDtypeStruct((2, count, passages), jnp.float32)] * 2
        + [jax.ShapeDtypeStruct((copies, 2, count), jnp.float32)],
        in_specs=[space] * 8,
        out_specs=[space] * 3,
        scratch_shapes=[pltpu.VMEM((len(parts), each, width), jnp.bfloat16)],
        cost_estimate=pl.CostEstimate(
            flops=8 * count * passages * width,
            bytes_accessed=8 * passages * width,
            transcendentals=4 * count * passages,
        ),
        compiler_params=pltpu.CompilerParams(vmem_limit_bytes=16 * 1024 * 1024),
    )(*parts, *blocks)


def arrange_kernel(sizes, kept_ref, crossed_ref, given_ref, out_ref, by_owner, placed):
    xh, yh, yl, zh, zl, tensor = sizes
    me = lax.axis_index(XL) * 2 + lax.axis_index(C)
    for flip, ref in enumerate(
        (kept_ref.at[0], given_ref.at[0], crossed_ref.at[0], given_ref.at[1])
    ):
        for half in range(placed.shape[0]):
            by_owner[me ^ flip, half] = ref[:, pl.ds(half * 128, 128)]
    for t in range(tensor):
        for near in range(yl * zl):
            y0, z0 = near // zl, near % zl
            for y1 in range(yh):
                for x in range(xh):
                    start = (near * yh + y1) * zh * xh + x
                    to = ((x * yh + y1) * yl + y0) * zh * zl + z0
                    for half in range(placed.shape[0]):
                        placed[half, pl.ds(to * tensor + t, zh, stride=zl * tensor)] = by_owner[
                            t, half, pl.ds(start, zh, stride=xh)
                        ]
    for half in range(placed.shape[0]):
        out_ref[:, pl.ds(half * 128, 128)] = placed[half]


def arrange(kept, crossed, given, sizes):
    _, rows, passages = kept.shape
    tensor = sizes[-1]
    space = pl.BlockSpec(memory_space=pltpu.VMEM)
    return pl.pallas_call(
        functools.partial(arrange_kernel, sizes),
        name="arrange",
        out_shape=jax.ShapeDtypeStruct((rows * tensor, passages), jnp.float32),
        in_specs=[space] * 3,
        out_specs=space,
        scratch_shapes=[
            pltpu.VMEM((tensor, passages // 128, rows, 128), jnp.float32),
            pltpu.VMEM((passages // 128, rows * tensor, 128), jnp.float32),
        ],
        compiler_params=pltpu.CompilerParams(vmem_limit_bytes=8 * 1024 * 1024),
    )(kept, crossed, given)


def step(q_states, k_states, v_states, residual, out_weight, final_gain, passages, lengths):
    xh, yh, yl, zh, zl, xl, c = (lax.axis_size(axis) for axis in CORPUS_TENSOR)
    tensor = xl * c
    width = out_weight.shape[1]
    terms = project(q_states, k_states, v_states, residual, out_weight, lengths, xh * tensor)

    terms = lax.all_to_all(terms, (XH, XL, C), 0, 0, tiled=True)

    across = swap(passages, XL)
    partner = swap(passages, C)
    both = swap(across, C)

    embed = embed_rows(terms, final_gain, xh, yh * zh)
    gathered = lax.all_to_all(embed, (YH, ZH), 0, 0, tiled=True).reshape(-1, width)
    shift = functools.partial(shifted, gathered)
    near_both = shift((YH, YL, ZH, ZL), 1, 1)
    near_y = shift((YH, YL, ZH, ZL), -1, 0)
    near_z = shift((YH, YL, ZH, ZL), 0, -1)

    held = hold((passages, partner, across))

    kept, crossing, stats = score_blocks(
        (gathered, near_z, near_y, near_both), (*held, both), zh * zl * c
    )

    crossed = swap(crossing, XL)
    given = swap(jnp.stack([kept[1], crossed[1]]), C)
    scores = arrange(kept, crossed, given, (xh, yh, yl, zh, zl, tensor))

    pairs = lax.all_to_all(stats, (ZH, ZL, C), 0, 0, tiled=True)
    pairs = lax.all_to_all(merge(pairs, c, xh * yh * yl * xl), (XH, YH, YL, XL), 0, 0, tiled=True)
    return scores, finish(pairs, (xh, yh, yl, zh, zl, xl, c))


def solution(mesh):
    split = Mesh(mesh.devices.reshape(2, 4, 2, 6, 2, 2, 2), CORPUS_TENSOR)
    in_specs = (
        P(CORPUS, TENSOR),
        P(CORPUS, TENSOR),
        P(CORPUS, TENSOR),
        P(CORPUS, None),
        P(TENSOR, None),
        P(),
        P(CORPUS_TENSOR, None),
        P(CORPUS),
    )
    out_specs = (P(None, CORPUS_TENSOR), P())
    return jax.shard_map(step, mesh=split, in_specs=in_specs, out_specs=out_specs, check_vma=False)
```
